32 devices in a mesh: row: 4 (over z), col: 8 (over y, x, core).
Axes of the slice: x: 2, y: 2, z: 4, core: 2. Of those that a mesh axis runs over, the one named last changes fastest.
Arguments:
- latent: float32 [2, 1024, 2048], P(None, 'row', 'col'), may hold values from -3 to 3
- momentum: float32 [2, 1024, 2048], P(None, 'row', 'col'), may hold values from -4 to 4
- hyper_params: float32 [2, 2], replicated, may hold values from 0.3 to 0.7
- velocity: float32 [2, 2], replicated, may hold values from -3 to 3
- step_size: float32 [2], replicated, may hold values from 0.08 to 0.12
- counts: int32 [1024, 2048], P('row', 'col'), may hold values from 0 to 7
- kappa_field: float32 [1024, 2048], P('row', 'col'), may hold values from 0.1 to 1
Outputs:
- latent_out: float32 [2, 1024, 2048], P(None, 'row', 'col')
- momentum_out: float32 [2, 1024, 2048], P(None, 'row', 'col')
- hyper_out: float32 [2, 2], replicated
- velocity_out: float32 [2, 2], replicated
The draws below stay inside these ranges and needn't reach their ends.
All inputs are finite; a program needn't handle non-finite values.
Results may differ from the reference program's by a relative error of at most 0.0001.
Values sent between devices are 32-bit elements; how exact they have to be, the bound alone decides.
A program may use at most 64 MiB of HBM per device.

```python
import math
import jax
import jax.numpy as jnp
from jax import lax

CHAINS = 2
STEPS = 10
NR = 1024
NC = 2048


def draw_latent(key, part):
    values = jax.random.uniform(key, (CHAINS, NR, NC), jnp.float32, -3.0, 3.0)
    return values


def draw_counts(key, part):
    columns = jnp.arange(NC, dtype=jnp.int32)
    ceiling = jnp.broadcast_to(3 + 6 * columns // NC, (NR, NC))
    return jax.random.randint(key, (NR, NC), 0, ceiling, dtype=jnp.int32)


def levels(stream_key, extent, cuts, low, high):
    level = 1.0
    for position, blocks in cuts:
        draws = jax.random.uniform(jax.random.fold_in(jax.random.fold_in(stream_key, 6), position), (blocks,), jnp.float32, low / len(cuts), high / len(cuts))
        level = level * jnp.repeat(jnp.exp(draws), extent[position] // blocks).reshape((-1,) + (1,) * (len(extent) - 1 - position))
    return level


def bell_draw(rng, extent, scale, bound, held_as=jnp.bfloat16):
    array = jax.random.normal(rng, extent, jnp.float32) * scale
    return jnp.minimum(jnp.maximum(array, -bound), bound).astype(held_as)


def setup_inputs(seed: int = 0) -> dict:
    seeds = jax.random.split(jax.random.key(seed), 8)
    latent = draw_latent(jax.random.fold_in(seeds[7], 71), 0)
    momentum = jnp.clip(jax.random.uniform(seeds[1], (CHAINS, NR, NC), jnp.float32, -4.0, 4.0) * levels(seeds[1], (CHAINS, NR, NC), ((1, 4), (2, 8)), -0.4, 0.0), -4.0, 4.0)
    hyper_params = jnp.clip(jax.random.uniform(seeds[2], (2, CHAINS), jnp.float32, 0.3, 0.7), 0.3, 0.7)
    velocity = bell_draw(seeds[3], (2, CHAINS), 0.3, 3.0, jnp.float32)
    step_size = jnp.clip(jnp.exp(jax.random.uniform(seeds[4], (CHAINS,), jnp.float32, math.log(0.08), math.log(0.12))), 0.08, 0.12)
    counts = draw_counts(jax.random.fold_in(seeds[7], 71), 0)
    kappa_field = jnp.clip(jnp.exp(math.log(1.0) - 2.3025851 * jax.random.uniform(seeds[6], (NR, NC), jnp.float32) ** levels(seeds[6], (NR, NC), ((0, 4), (1, 8)), -0.2, 0.2)), 0.1, 1.0)
    return {"latent": latent, "momentum": momentum, "hyper_params": hyper_params, "velocity": velocity, "step_size": step_size, "counts": counts, "kappa_field": kappa_field}


def stencil(field):
    return jnp.roll(field, 1, 0) + jnp.roll(field, -1, 0) + jnp.roll(field, 1, 1) + jnp.roll(field, -1, 1)


def reference(latent, momentum, hyper_params, velocity, step_size, counts, kappa_field):
    count_float = counts.astype(jnp.float32)
    total = float(NR * NC)

    def gradient_at(field, params):
        tau_value = jnp.exp(params[1])
        applied = (kappa_field + 4.0) * field - stencil(field)
        intensity = jnp.exp(params[0] + field)
        gradient = tau_value * applied - count_float + intensity
        quadratic = jnp.sum(field * applied)
        excess = jnp.sum(intensity - count_float)
        accel = jnp.stack([excess / total, 0.5 * tau_value * quadratic / total - 0.5])
        return gradient, accel

    def single_chain(inputs):
        field, moment, params, speed, size_value = inputs
        gradient, accel = gradient_at(field, params)
        for index_step in range(STEPS):
            moment = moment - 0.5 * size_value * gradient
            speed = speed - 0.5 * size_value * accel
            field = field + size_value * moment
            params = params + size_value * speed
            gradient, accel = gradient_at(field, params)
            moment = moment - 0.5 * size_value * gradient
            speed = speed - 0.5 * size_value * accel
        return field, moment, params, speed

    results = lax.map(single_chain, (latent, momentum, hyper_params.T, velocity.T, step_size))
    return results[0], results[1], results[2].T, results[3].T
```

```python
import functools

import jax
import jax.numpy as jnp
from jax import lax
from jax.experimental import pallas as pl
from jax.experimental.pallas import tpu as pltpu
from jax.sharding import PartitionSpec as P

STEPS = 10
HALO = 16
PAD = 8
TOP = PAD + HALO
LANES = 128
SEG = 16
MESH = pl.DeviceIdType.MESH


def kernel(
    sizes, latent, momentum, counts, kappa, hyper, velocity, step_size,
    latent_out, momentum_out, hyper_out, velocity_out,
    state, applied, intensity, raw_counts, left_pack, right_pack, from_right, from_left,
    payload, gathered,
    load_sem, store_sem, halo_send, halo_recv, sum_send, sum_recv,
):
    nr, nc, chains, rows, tiles, total = sizes
    devices = nr * nc
    row, col = lax.axis_index("row"), lax.axis_index("col")
    me = row * nc + col
    arrays = 2 * chains + 2
    kap, cnt = 2 * chains, 2 * chains + 1
    own = pl.ds(TOP, rows)

    loads = []
    for c in range(chains):
        for j in range(tiles):
            cols = pl.ds(j * LANES, LANES)
            loads.append((latent.at[c, :, cols], state.at[c, j, own, :]))
            loads.append((momentum.at[c, :, cols], state.at[chains + c, j, own, :]))
    for j in range(tiles):
        cols = pl.ds(j * LANES, LANES)
        loads.append((kappa.at[:, cols], state.at[kap, j, own, :]))
        loads.append((counts.at[:, cols], raw_counts.at[j]))
    loads = [pltpu.make_async_copy(s, d, load_sem.at[i]) for i, (s, d) in enumerate(loads)]
    for copy in loads:
        copy.start()

    def peer(d):
        other = lax.rem(me + d, devices)
        return (other // nc, lax.rem(other, nc))

    barrier = pltpu.get_barrier_semaphore()
    for d in range(1, devices):
        pl.semaphore_signal(barrier, inc=1, device_id=peer(d), device_id_type=MESH)

    lane = lax.broadcasted_iota(jnp.int32, (8, LANES), 1)
    seg = lane // SEG
    sublane = lax.broadcasted_iota(jnp.int32, (8, LANES), 0)
    first, last = lane == 0, lane == LANES - 1

    for copy in loads:
        copy.wait()

    def pack(i, counted):
        rel = pl.multiple_of(i * 8, 8)
        r = pl.multiple_of(TOP + i * 8, 8)
        for j in range(tiles):
            value = raw_counts[j, pl.ds(rel, 8), :].astype(jnp.float32)
            state[cnt, j, pl.ds(r, 8), :] = value
            counted = counted + value
        lp = state[0, 0, pl.ds(r, 8), :]
        rp = pltpu.roll(state[0, tiles - 1, pl.ds(r, 8), :], SEG, 1)
        for a in range(1, arrays):
            lp = jnp.where(seg == a, pltpu.roll(state[a, 0, pl.ds(r, 8), :], SEG * a, 1), lp)
            rolled = pltpu.roll(state[a, tiles - 1, pl.ds(r, 8), :], SEG * (a + 1) % LANES, 1)
            rp = jnp.where(seg == a, rolled, rp)
        left_pack[pl.ds(rel, 8), :] = lp
        right_pack[pl.ds(rel, 8), :] = rp
        return counted

    counted = lax.fori_loop(0, rows // 8, pack, jnp.zeros((8, LANES), jnp.float32))

    pl.semaphore_wait(barrier, devices - 1)

    up, down = lax.rem(row + nr - 1, nr), lax.rem(row + 1, nr)
    left, right = lax.rem(col + nc - 1, nc), lax.rem(col + 1, nc)
    head, tail = pl.ds(0, HALO), pl.ds(rows - HALO, HALO)
    body, below = pl.ds(HALO, rows), pl.ds(HALO + rows, HALO)
    halos = [
        (left_pack.at[:, :], from_right.at[body, :], (row, left)),
        (right_pack.at[:, :], from_left.at[body, :], (row, right)),
        (
            state.at[:, pl.ds(0, tiles), pl.ds(TOP, HALO), :],
            state.at[:, pl.ds(0, tiles), pl.ds(TOP + rows, HALO), :],
            (up, col),
        ),
        (
            state.at[:, pl.ds(0, tiles), pl.ds(TOP + rows - HALO, HALO), :],
            state.at[:, pl.ds(0, tiles), pl.ds(PAD, HALO), :],
            (down, col),
        ),
        (left_pack.at[tail, :], from_right.at[head, :], (down, left)),
        (left_pack.at[head, :], from_right.at[below, :], (up, left)),
        (right_pack.at[tail, :], from_left.at[head, :], (down, right)),
        (right_pack.at[head, :], from_left.at[below, :], (up, right)),
    ]
    halos = [
        pltpu.make_async_remote_copy(
            src_ref=s, dst_ref=d, send_sem=halo_send.at[i], recv_sem=halo_recv.at[i],
            device_id=where, device_id_type=MESH,
        )
        for i, (s, d, where) in enumerate(halos)
    ]
    for copy in halos:
        copy.start()
    for copy in halos:
        copy.wait()

    def unpack(i, carry):
        rel = pl.multiple_of(i * 8, 8)
        r = pl.multiple_of(PAD + i * 8, 8)
        fr = from_right[pl.ds(rel, 8), :]
        fl = from_left[pl.ds(rel, 8), :]
        for a in range(arrays):
            right_part = pltpu.roll(fr, (LANES - SEG * a) % LANES, 1)
            left_part = pltpu.roll(fl, (LANES - SEG * (a + 1)) % LANES, 1)
            value = jnp.where(seg == 0, right_part, jnp.where(seg == 7, left_part, 0.0))
            state[a, tiles, pl.ds(r, 8), :] = value
        return carry

    lax.fori_loop(0, (rows + 2 * HALO) // 8, unpack, 0)

    def stencil_tiles(r, lane_tiles):
        rowset = pl.ds(r, 8)
        terms = []
        for c in range(chains):
            full = [state[c, j, rowset, :] for j in range(tiles + 1)]
            to_right = [pltpu.roll(x, 1, 1) for x in full]
            to_left = [pltpu.roll(x, LANES - 1, 1) for x in full]
            quad = mass = None
            for j in lane_tiles:
                v = full[j]
                beside = jnp.where(first, to_right[j - 1], to_right[j])
                beside += jnp.where(last, to_left[(j + 1) % (tiles + 1)], to_left[j])
                beside += state[c, j, pl.ds(r - 1, 8), :] + state[c, j, pl.ds(r + 1, 8), :]
                av = (state[kap, j, rowset, :] + 4.0) * v - beside
                ex = jnp.exp(v)
                applied[c, j, rowset, :] = av
                intensity[c, j, rowset, :] = ex
                quad = v * av if quad is None else quad + v * av
                mass = ex if mass is None else mass + ex
            terms += [quad, mass]
        return terms

    def own_part():
        def body(i, sums):
            r = pl.multiple_of(TOP + i * 8, 8)
            return tuple(s + t for s, t in zip(sums, stencil_tiles(r, range(tiles))))

        zero = jnp.zeros((8, LANES), jnp.float32)
        return lax.fori_loop(0, rows // 8, body, (zero,) * (2 * chains))

    def halo_part():
        def side(i, carry):
            stencil_tiles(pl.multiple_of(TOP + i * 8, 8), [tiles])
            return carry

        def ends(i, carry):
            shift = jnp.where(i < HALO // 8, PAD, PAD + rows)
            stencil_tiles(pl.multiple_of(shift + i * 8, 8), range(tiles + 1))
            return carry

        lax.fori_loop(0, rows // 8, side, 0)
        lax.fori_loop(0, 2 * HALO // 8, ends, 0)

    def whole(x):
        return jnp.sum(jnp.sum(x, axis=0, keepdims=True), axis=1, keepdims=True)

    counted = whole(counted)

    def send(k, sums):
        q0, e0, q1, e1 = [whole(s) for s in sums]
        out = counted
        for i, value in enumerate((q0, q1, e0, e1)):
            out = jnp.where(seg[:1] == i, value, out)
        payload[k] = out
        gathered[k, me] = out
        for d in range(1, devices):
            pltpu.make_async_remote_copy(
                src_ref=payload.at[k], dst_ref=gathered.at[k, me],
                send_sem=sum_send.at[k], recv_sem=sum_recv.at[k],
                device_id=peer(d), device_id_type=MESH,
            ).start()

    def collect(k):
        bulk = gathered.at[k, pl.ds(0, devices - 1)]
        copy = pltpu.make_async_remote_copy(
            src_ref=bulk, dst_ref=bulk, send_sem=sum_send.at[k], recv_sem=sum_recv.at[k],
            device_id=peer(1), device_id_type=MESH,
        )
        copy.wait_recv()
        copy.wait_send()
        return jnp.broadcast_to(jnp.sum(gathered[k], axis=0), (8, LANES))

    def spread(values):
        out = jnp.zeros((8, LANES), jnp.float32)
        for i, value in enumerate(values):
            out = jnp.where(seg == i, value, out)
        return out

    h = [step_size[c] for c in range(chains)]
    hvec = spread([h[0], h[1], h[0], h[1]])
    hyp = spread([hyper[1, 0], hyper[1, 1], hyper[0, 0], hyper[0, 1]])
    vel = spread([velocity[1, 0], velocity[1, 1], velocity[0, 0], velocity[0, 1]])
    is_quad = seg < 2
    coef = jnp.where(is_quad, 0.5 / total, 1.0 / total)

    def accel(summed, expd):
        target = pltpu.roll(summed, LANES - 2 * SEG, 1) * (1.0 / total)
        return coef * expd * summed - jnp.where(is_quad, 0.5, target)

    def pick(x, i):
        return jnp.sum(jnp.where(lane == i * SEG, x, 0.0), axis=1, keepdims=True)

    def weights(expd, scale):
        scaled = expd * hvec * scale
        return [jnp.broadcast_to(pick(scaled, i), (8, LANES)) for i in range(2 * chains)]

    def kick(r, c, j, w, scale):
        rowset = pl.ds(r, 8)
        m = state[chains + c, j, rowset, :] + (h[c] * scale) * state[cnt, j, rowset, :]
        m = m - w[c] * applied[c, j, rowset, :] - w[chains + c] * intensity[c, j, rowset, :]
        state[chains + c, j, rowset, :] = m
        return m

    def advance(w, scale):
        def body(i, carry):
            r = pl.multiple_of(PAD + i * 8, 8)
            for c in range(chains):
                for j in range(tiles + 1):
                    m = kick(r, c, j, w, scale)
                    state[c, j, pl.ds(r, 8), :] += h[c] * m
            return carry

        lax.fori_loop(0, (rows + 2 * HALO) // 8, body, 0)

    def round_of(k):
        sums = own_part()
        send(k, sums)

    expd = jnp.exp(hyp)
    round_of(0)
    halo_part()
    advance(weights(expd, 0.5), 0.5)
    round_of(1)

    def step(k, carry):
        hyp, vel, expd = carry
        halo_part()
        a = accel(collect(k - 1), expd)
        vel = vel - jnp.where(k == 1, 0.5, 1.0) * hvec * a
        hyp = hyp + hvec * vel
        expd = jnp.exp(hyp)
        advance(weights(expd, 1.0), 1.0)
        round_of(k + 1)
        return hyp, vel, expd

    hyp, vel, expd = lax.fori_loop(1, STEPS, step, (hyp, vel, expd))

    def stores(base, out, start):
        copies = []
        for c in range(chains):
            for j in range(tiles):
                cols = pl.ds(j * LANES, LANES)
                copies.append(
                    pltpu.make_async_copy(
                        state.at[base + c, j, own, :],
                        out.at[c, :, cols],
                        store_sem.at[start + len(copies)],
                    )
                )
        for copy in copies:
            copy.start()
        return copies

    pending = stores(0, latent_out, 0)
    vel = vel - hvec * accel(collect(STEPS - 1), expd)
    hyp = hyp + hvec * vel
    expd = jnp.exp(hyp)
    w = weights(expd, 0.5)

    def final(i, carry):
        r = pl.multiple_of(TOP + i * 8, 8)
        for c in range(chains):
            for j in range(tiles):
                kick(r, c, j, w, 0.5)
        return carry

    lax.fori_loop(0, rows // 8, final, 0)
    pending += stores(chains, momentum_out, len(pending))
    vel = vel - 0.5 * hvec * accel(collect(STEPS), expd)

    out_row, out_col = sublane[:2, :2], lane[:2, :2]
    for x, ref in ((hyp, hyper_out), (vel, velocity_out)):
        picks = [pick(x, i)[:2] for i in range(2 * chains)]
        low = jnp.where(out_col == 0, picks[2], picks[3])
        high = jnp.where(out_col == 0, picks[0], picks[1])
        ref[...] = jnp.where(out_row == 0, low, high)
    for copy in pending:
        copy.wait()


def solution(mesh):
    nr, nc = mesh.shape["row"], mesh.shape["col"]
    devices = nr * nc

    def shards(latent, momentum, hyper_params, velocity, step_size, counts, kappa_field):
        chains, rows, cols = latent.shape
        tiles = cols // LANES
        deep = rows + 2 * TOP
        total = float(rows * nr * cols * nc)
        sizes = (nr, nc, chains, rows, tiles, total)
        anywhere = pl.BlockSpec(memory_space=pl.ANY)
        scalars = pl.BlockSpec(memory_space=pltpu.SMEM)
        small = pl.BlockSpec(memory_space=pltpu.VMEM)
        arrays = 2 * chains + 2
        f32 = jnp.float32
        return pl.pallas_call(
            functools.partial(kernel, sizes),
            out_shape=(
                jax.ShapeDtypeStruct(latent.shape, f32),
                jax.ShapeDtypeStruct(latent.shape, f32),
                jax.ShapeDtypeStruct(hyper_params.shape, f32),
                jax.ShapeDtypeStruct(velocity.shape, f32),
            ),
            in_specs=[anywhere] * 4 + [scalars] * 3,
            out_specs=(anywhere, anywhere, small, small),
            scratch_shapes=[
                pltpu.VMEM((arrays, tiles + 1, deep, LANES), f32),
                pltpu.VMEM((chains, tiles + 1, deep, LANES), f32),
                pltpu.VMEM((chains, tiles + 1, deep, LANES), f32),
                pltpu.VMEM((tiles, rows, LANES), jnp.int32),
                pltpu.VMEM((rows, LANES), f32),
                pltpu.VMEM((rows, LANES), f32),
                pltpu.VMEM((rows + 2 * HALO, LANES), f32),
                pltpu.VMEM((rows + 2 * HALO, LANES), f32),
                pltpu.VMEM((STEPS + 1, 1, LANES), f32),
                pltpu.VMEM((STEPS + 1, devices, 1, LANES), f32),
                pltpu.SemaphoreType.DMA((2 * tiles * (chains + 1),)),
                pltpu.SemaphoreType.DMA((2 * tiles * chains,)),
                pltpu.SemaphoreType.DMA((8,)),
                pltpu.SemaphoreType.DMA((8,)),
                pltpu.SemaphoreType.DMA((STEPS + 1,)),
                pltpu.SemaphoreType.DMA((STEPS + 1,)),
            ],
            compiler_params=pltpu.CompilerParams(collective_id=0, has_side_effects=True),
        )(latent, momentum, counts, kappa_field, hyper_params, velocity, step_size)

    placed = (
        P(None, "row", "col"),
        P(None, "row", "col"),
        P(),
        P(),
        P(),
        P("row", "col"),
        P("row", "col"),
    )
    return jax.shard_map(
        shards,
        mesh=mesh,
        in_specs=placed,
        out_specs=(P(None, "row", "col"), P(None, "row", "col"), P(), P()),
        check_vma=False,
    )
```

```python
import functools

import jax
import jax.numpy as jnp
from jax import lax
from jax.experimental import pallas as pl
from jax.experimental.pallas import tpu as pltpu
from jax.sharding import PartitionSpec as P

STEPS = 10
HALO = 16
PAD = 8
TOP = PAD + HALO
LANES = 128
OWN_DEEP, SIDE_DEEP, KICK_DEEP, PACK_DEEP, UNPACK_DEEP = 128, 128, 32, 64, 96
SEG = 16
MESH = pl.DeviceIdType.MESH


def kernel(
    sizes, latent, momentum, counts, kappa, hyper, velocity, step_size,
    latent_out, momentum_out, hyper_out, velocity_out,
    state, diagonal, applied, intensity, raw_counts, left_pack, right_pack, from_right, from_left,
    payload, gathered,
    load_sem, store_sem, halo_send, halo_recv, sum_send, sum_recv,
):
    nr, nc, chains, rows, tiles, total = sizes
    devices = nr * nc
    row, col = lax.axis_index("row"), lax.axis_index("col")
    me = row * nc + col
    arrays = 2 * chains + 2
    kap, cnt = 2 * chains, 2 * chains + 1
    own = pl.ds(TOP, rows)

    loads = []
    for c in range(chains):
        for j in range(tiles):
            cols = pl.ds(j * LANES, LANES)
            loads.append((latent.at[c, :, cols], state.at[c, j, own, :]))
            loads.append((momentum.at[c, :, cols], state.at[chains + c, j, own, :]))
    for j in range(tiles):
        cols = pl.ds(j * LANES, LANES)
        loads.append((kappa.at[:, cols], state.at[kap, j, own, :]))
        loads.append((counts.at[:, cols], raw_counts.at[j]))
    loads = [pltpu.make_async_copy(s, d, load_sem.at[i]) for i, (s, d) in enumerate(loads)]
    for copy in loads:
        copy.start()

    def peer(d):
        other = lax.rem(me + d, devices)
        return (other // nc, lax.rem(other, nc))

    barrier = pltpu.get_barrier_semaphore()
    for d in range(1, devices):
        pl.semaphore_signal(barrier, inc=1, device_id=peer(d), device_id_type=MESH)

    lane = lax.broadcasted_iota(jnp.int32, (8, LANES), 1)
    seg = lane // SEG
    sublane = lax.broadcasted_iota(jnp.int32, (8, LANES), 0)
    first = lax.broadcasted_iota(jnp.int32, (1, LANES), 1) == 0
    last = lax.broadcasted_iota(jnp.int32, (1, LANES), 1) == LANES - 1

    for copy in loads:
        copy.wait()

    def pack(i, counted):
        rel = pl.ds(pl.multiple_of(i * PACK_DEEP, 8), PACK_DEEP)
        here = pl.ds(pl.multiple_of(TOP + i * PACK_DEEP, 8), PACK_DEEP)
        value = [raw_counts[j, rel, :].astype(jnp.float32) for j in range(tiles)]
        heads = [state[a, 0, here, :] for a in range(arrays - 1)] + [value[0]]
        tails = [state[a, tiles - 1, here, :] for a in range(arrays - 1)] + [value[-1]]
        lp, rp = heads[0], pltpu.roll(tails[0], SEG, 1)
        for a in range(1, arrays):
            lp = jnp.where(seg[:1] == a, pltpu.roll(heads[a], SEG * a, 1), lp)
            rp = jnp.where(seg[:1] == a, pltpu.roll(tails[a], SEG * (a + 1) % LANES, 1), rp)
        left_pack[rel, :] = lp
        right_pack[rel, :] = rp
        for j in range(tiles):
            state[cnt, j, here, :] = value[j]
        both = sum(value)
        return counted + sum(both[8 * u : 8 * u + 8] for u in range(PACK_DEEP // 8))

    zeros = jnp.zeros((8, LANES), jnp.float32)
    counted = lax.fori_loop(0, rows // PACK_DEEP, pack, zeros)

    pl.semaphore_wait(barrier, devices - 1)

    up, down = lax.rem(row + nr - 1, nr), lax.rem(row + 1, nr)
    left, right = lax.rem(col + nc - 1, nc), lax.rem(col + 1, nc)
    head, tail = pl.ds(0, HALO), pl.ds(rows - HALO, HALO)
    body, below = pl.ds(HALO, rows), pl.ds(HALO + rows, HALO)
    halos = [
        (left_pack.at[:, :], from_right.at[body, :], (row, left)),
        (right_pack.at[:, :], from_left.at[body, :], (row, right)),
        (
            state.at[:, pl.ds(0, tiles), pl.ds(TOP, HALO), :],
            state.at[:, pl.ds(0, tiles), pl.ds(TOP + rows, HALO), :],
            (up, col),
        ),
        (
            state.at[:, pl.ds(0, tiles), pl.ds(TOP + rows - HALO, HALO), :],
            state.at[:, pl.ds(0, tiles), pl.ds(PAD, HALO), :],
            (down, col),
        ),
        (left_pack.at[tail, :], from_right.at[head, :], (down, left)),
        (left_pack.at[head, :], from_right.at[below, :], (up, left)),
        (right_pack.at[tail, :], from_left.at[head, :], (down, right)),
        (right_pack.at[head, :], from_left.at[below, :], (up, right)),
    ]
    halos = [
        pltpu.make_async_remote_copy(
            src_ref=s, dst_ref=d, send_sem=halo_send.at[i], recv_sem=halo_recv.at[i],
            device_id=where, device_id_type=MESH,
        )
        for i, (s, d, where) in enumerate(halos)
    ]
    for copy in halos:
        copy.start()
    for copy in halos:
        copy.wait()

    def unpack(i, carry):
        rel = pl.ds(pl.multiple_of(i * UNPACK_DEEP, 8), UNPACK_DEEP)
        here = pl.ds(pl.multiple_of(PAD + i * UNPACK_DEEP, 8), UNPACK_DEEP)
        fr, fl = from_right[rel, :], from_left[rel, :]
        values = []
        for a in range(arrays):
            right_part = pltpu.roll(fr, (LANES - SEG * a) % LANES, 1) if a else fr
            left_part = pltpu.roll(fl, (LANES - SEG * (a + 1)) % LANES, 1)
            left_part = jnp.where(seg[:1] == 7, left_part, 0.0)
            values.append(jnp.where(seg[:1] == 0, right_part, left_part))
        plus = [state[kap, j, here, :] + 4.0 for j in range(tiles)] + [values[kap] + 4.0]
        for a in range(arrays):
            state[a, tiles, here, :] = values[a]
        for j in range(tiles + 1):
            diagonal[j, here, :] = plus[j]
        return carry

    lax.fori_loop(0, (rows + 2 * HALO) // UNPACK_DEEP, unpack, 0)

    def stencil_tiles(r, deep, lane_tiles):
        rowset = pl.ds(r, deep)
        terms, results = [], []
        for c in range(chains):
            full = [state[c, j, rowset, :] for j in range(tiles + 1)]
            used = sorted({(j + s) % (tiles + 1) for j in lane_tiles for s in (-1, 0)})
            to_right = {j: pltpu.roll(full[j], 1, 1) for j in used}
            used = sorted({(j + s) % (tiles + 1) for j in lane_tiles for s in (1, 0)})
            to_left = {j: pltpu.roll(full[j], LANES - 1, 1) for j in used}
            quad = mass = None
            for j in lane_tiles:
                v = full[j]
                beside = jnp.where(first, to_right[(j - 1) % (tiles + 1)], to_right[j])
                beside += jnp.where(last, to_left[(j + 1) % (tiles + 1)], to_left[j])
                beside += state[c, j, pl.ds(r - 1, deep), :] + state[c, j, pl.ds(r + 1, deep), :]
                av = diagonal[j, rowset, :] * v - beside
                ex = jnp.exp(v)
                results.append((c, j, av, ex))
                quad = v * av if quad is None else quad + v * av
                mass = ex if mass is None else mass + ex
            terms += [quad, mass]
        for c, j, av, ex in results:
            applied[c, j, rowset, :] = av
            intensity[c, j, rowset, :] = ex
        return [sum(t[8 * u : 8 * u + 8] for u in range(deep // 8)) for t in terms]

    def own_part():
        def body(i, sums):
            r = pl.multiple_of(TOP + i * OWN_DEEP, 8)
            terms = stencil_tiles(r, OWN_DEEP, range(tiles))
            return tuple(s + t for s, t in zip(sums, terms))

        zero = jnp.zeros((8, LANES), jnp.float32)
        return lax.fori_loop(0, rows // OWN_DEEP, body, (zero,) * (2 * chains))

    def halo_part():
        def side(i, carry):
            stencil_tiles(pl.multiple_of(TOP + i * SIDE_DEEP, 8), SIDE_DEEP, [tiles])
            return carry

        lax.fori_loop(0, rows // SIDE_DEEP, side, 0)
        stencil_tiles(PAD, HALO, range(tiles + 1))
        stencil_tiles(TOP + rows, HALO, range(tiles + 1))

    def whole(x):
        return jnp.sum(jnp.sum(x, axis=0, keepdims=True), axis=1, keepdims=True)

    counted = whole(counted)

    def send(k, sums):
        q0, e0, q1, e1 = [whole(s) for s in sums]
        out = counted
        for i, value in enumerate((q0, q1, e0, e1)):
            out = jnp.where(seg[:1] == i, value, out)
        payload[k] = out
        gathered[k, me] = out
        for d in range(1, devices):
            pltpu.make_async_remote_copy(
                src_ref=payload.at[k], dst_ref=gathered.at[k, me],
                send_sem=sum_send.at[k], recv_sem=sum_recv.at[k],
                device_id=peer(d), device_id_type=MESH,
            ).start()

    def collect(k):
        bulk = gathered.at[k, pl.ds(0, devices - 1)]
        copy = pltpu.make_async_remote_copy(
            src_ref=bulk, dst_ref=bulk, send_sem=sum_send.at[k], recv_sem=sum_recv.at[k],
            device_id=peer(1), device_id_type=MESH,
        )
        copy.wait_recv()
        copy.wait_send()
        return jnp.broadcast_to(jnp.sum(gathered[k], axis=0), (8, LANES))

    def spread(values):
        out = jnp.zeros((8, LANES), jnp.float32)
        for i, value in enumerate(values):
            out = jnp.where(seg == i, value, out)
        return out

    h = [step_size[c] for c in range(chains)]
    hvec = spread([h[0], h[1], h[0], h[1]])
    hyp = spread([hyper[1, 0], hyper[1, 1], hyper[0, 0], hyper[0, 1]])
    vel = spread([velocity[1, 0], velocity[1, 1], velocity[0, 0], velocity[0, 1]])
    is_quad = seg < 2
    coef = jnp.where(is_quad, 0.5 / total, 1.0 / total)

    def accel(summed, expd):
        target = pltpu.roll(summed, LANES - 2 * SEG, 1) * (1.0 / total)
        return coef * expd * summed - jnp.where(is_quad, 0.5, target)

    def pick(x, i):
        return jnp.sum(jnp.where(lane == i * SEG, x, 0.0), axis=1, keepdims=True)

    def weights(expd, scale):
        scaled = expd * hvec * scale
        return [jnp.broadcast_to(pick(scaled, i)[:1], (1, LANES)) for i in range(2 * chains)]

    def kick(r, deep, c, j, w, scale):
        rowset = pl.ds(r, deep)
        m = state[chains + c, j, rowset, :] + (h[c] * scale) * state[cnt, j, rowset, :]
        return m - w[c] * applied[c, j, rowset, :] - w[chains + c] * intensity[c, j, rowset, :]

    def advance(w, scale):
        def body(i, carry):
            rowset = pl.ds(pl.multiple_of(PAD + i * KICK_DEEP, 8), KICK_DEEP)
            moved = []
            for c in range(chains):
                for j in range(tiles + 1):
                    m = kick(rowset.start, KICK_DEEP, c, j, w, scale)
                    moved.append((c, j, m, state[c, j, rowset, :] + h[c] * m))
            for c, j, m, v in moved:
                state[chains + c, j, rowset, :] = m
                state[c, j, rowset, :] = v
            return carry

        lax.fori_loop(0, (rows + 2 * HALO) // KICK_DEEP, body, 0)

    def round_of(k):
        sums = own_part()
        send(k, sums)

    expd = jnp.exp(hyp)
    round_of(0)
    halo_part()
    advance(weights(expd, 0.5), 0.5)
    round_of(1)

    def step(k, carry):
        hyp, vel, expd = carry
        halo_part()
        a = accel(collect(k - 1), expd)
        vel = vel - jnp.where(k == 1, 0.5, 1.0) * hvec * a
        hyp = hyp + hvec * vel
        expd = jnp.exp(hyp)
        advance(weights(expd, 1.0), 1.0)
        round_of(k + 1)
        return hyp, vel, expd

    hyp, vel, expd = lax.fori_loop(1, STEPS, step, (hyp, vel, expd))

    def stores(base, out, start):
        copies = []
        for c in range(chains):
            for j in range(tiles):
                cols = pl.ds(j * LANES, LANES)
                copies.append(
                    pltpu.make_async_copy(
                        state.at[base + c, j, own, :],
                        out.at[c, :, cols],
                        store_sem.at[start + len(copies)],
                    )
                )
        for copy in copies:
            copy.start()
        return copies

    pending = stores(0, latent_out, 0)
    vel = vel - hvec * accel(collect(STEPS - 1), expd)
    hyp = hyp + hvec * vel
    expd = jnp.exp(hyp)
    w = weights(expd, 0.5)

    def final(i, carry):
        rowset = pl.ds(pl.multiple_of(TOP + i * KICK_DEEP, 8), KICK_DEEP)
        moved = []
        for c in range(chains):
            for j in range(tiles):
                moved.append((c, j, kick(rowset.start, KICK_DEEP, c, j, w, 0.5)))
        for c, j, m in moved:
            state[chains + c, j, rowset, :] = m
        return carry

    lax.fori_loop(0, rows // KICK_DEEP, final, 0)
    pending += stores(chains, momentum_out, len(pending))
    vel = vel - 0.5 * hvec * accel(collect(STEPS), expd)

    out_row, out_col = sublane[:2, :2], lane[:2, :2]
    for x, ref in ((hyp, hyper_out), (vel, velocity_out)):
        picks = [pick(x, i)[:2] for i in range(2 * chains)]
        low = jnp.where(out_col == 0, picks[2], picks[3])
        high = jnp.where(out_col == 0, picks[0], picks[1])
        ref[...] = jnp.where(out_row == 0, low, high)
    for copy in pending:
        copy.wait()


def solution(mesh):
    nr, nc = mesh.shape["row"], mesh.shape["col"]
    devices = nr * nc

    def shards(latent, momentum, hyper_params, velocity, step_size, counts, kappa_field):
        chains, rows, cols = latent.shape
        tiles = cols // LANES
        deep = rows + 2 * TOP
        total = float(rows * nr * cols * nc)
        sizes = (nr, nc, chains, rows, tiles, total)
        anywhere = pl.BlockSpec(memory_space=pl.ANY)
        scalars = pl.BlockSpec(memory_space=pltpu.SMEM)
        small = pl.BlockSpec(memory_space=pltpu.VMEM)
        arrays = 2 * chains + 2
        f32 = jnp.float32
        return pl.pallas_call(
            functools.partial(kernel, sizes),
            out_shape=(
                jax.ShapeDtypeStruct(latent.shape, f32),
                jax.ShapeDtypeStruct(latent.shape, f32),
                jax.ShapeDtypeStruct(hyper_params.shape, f32),
                jax.ShapeDtypeStruct(velocity.shape, f32),
            ),
            in_specs=[anywhere] * 4 + [scalars] * 3,
            out_specs=(anywhere, anywhere, small, small),
            scratch_shapes=[
                pltpu.VMEM((arrays, tiles + 1, deep, LANES), f32),
                pltpu.VMEM((tiles + 1, deep, LANES), f32),
                pltpu.VMEM((chains, tiles + 1, deep, LANES), f32),
                pltpu.VMEM((chains, tiles + 1, deep, LANES), f32),
                pltpu.VMEM((tiles, rows, LANES), jnp.int32),
                pltpu.VMEM((rows, LANES), f32),
                pltpu.VMEM((rows, LANES), f32),
                pltpu.VMEM((rows + 2 * HALO, LANES), f32),
                pltpu.VMEM((rows + 2 * HALO, LANES), f32),
                pltpu.VMEM((STEPS + 1, 1, LANES), f32),
                pltpu.VMEM((STEPS + 1, devices, 1, LANES), f32),
                pltpu.SemaphoreType.DMA((2 * tiles * (chains + 1),)),
                pltpu.SemaphoreType.DMA((2 * tiles * chains,)),
                pltpu.SemaphoreType.DMA((8,)),
                pltpu.SemaphoreType.DMA((8,)),
                pltpu.SemaphoreType.DMA((STEPS + 1,)),
                pltpu.SemaphoreType.DMA((STEPS + 1,)),
            ],
            compiler_params=pltpu.CompilerParams(collective_id=0, has_side_effects=True),
        )(latent, momentum, counts, kappa_field, hyper_params, velocity, step_size)

    placed = (
        P(None, "row", "col"),
        P(None, "row", "col"),
        P(),
        P(),
        P(),
        P("row", "col"),
        P("row", "col"),
    )
    return jax.shard_map(
        shards,
        mesh=mesh,
        in_specs=placed,
        out_specs=(P(None, "row", "col"), P(None, "row", "col"), P(), P()),
        check_vma=False,
    )
```

```python
import functools

import jax
import jax.numpy as jnp
from jax import lax
from jax.experimental import pallas as pl
from jax.experimental.pallas import tpu as pltpu
from jax.sharding import PartitionSpec as P

STEPS = 10
HALO = 16
PAD = 8
TOP = PAD + HALO
LANES = 128
OWN_DEEP, SIDE_DEEP, KICK_DEEP, PACK_DEEP, UNPACK_DEEP = 256, 256, 48, 64, 96
SEG = 16
MESH = pl.DeviceIdType.MESH


def kernel(
    sizes, latent, momentum, counts, kappa, hyper, velocity, step_size,
    latent_out, momentum_out, hyper_out, velocity_out,
    state, diagonal, applied, intensity, raw_counts, left_pack, right_pack, from_right, from_left,
    payload, gathered,
    load_sem, store_sem, halo_send, halo_recv, sum_send, sum_recv,
):
    nr, nc, chains, rows, tiles, total = sizes
    devices = nr * nc
    row, col = lax.axis_index("row"), lax.axis_index("col")
    me = row * nc + col
    arrays = 2 * chains + 2
    kap, cnt = 2 * chains, 2 * chains + 1
    own = pl.ds(TOP, rows)

    loads = []
    for c in range(chains):
        for j in range(tiles):
            cols = pl.ds(j * LANES, LANES)
            loads.append((latent.at[c, :, cols], state.at[c, j, own, :]))
            loads.append((momentum.at[c, :, cols], state.at[chains + c, j, own, :]))
    for j in range(tiles):
        cols = pl.ds(j * LANES, LANES)
        loads.append((kappa.at[:, cols], state.at[kap, j, own, :]))
        loads.append((counts.at[:, cols], raw_counts.at[j]))
    loads = [pltpu.make_async_copy(s, d, load_sem.at[i]) for i, (s, d) in enumerate(loads)]
    for copy in loads:
        copy.start()

    def peer(d):
        other = lax.rem(me + d, devices)
        return (other // nc, lax.rem(other, nc))

    barrier = pltpu.get_barrier_semaphore()
    for d in sorted(range(1, devices), key=lambda d: -min(d, devices - d)):
        pl.semaphore_signal(barrier, inc=1, device_id=peer(d), device_id_type=MESH)

    lane = lax.broadcasted_iota(jnp.int32, (8, LANES), 1)
    seg = lane // SEG
    sublane = lax.broadcasted_iota(jnp.int32, (8, LANES), 0)
    first = lax.broadcasted_iota(jnp.int32, (1, LANES), 1) == 0
    last = lax.broadcasted_iota(jnp.int32, (1, LANES), 1) == LANES - 1

    for copy in loads:
        copy.wait()

    def pack(i, counted):
        rel = pl.ds(pl.multiple_of(i * PACK_DEEP, 8), PACK_DEEP)
        here = pl.ds(pl.multiple_of(TOP + i * PACK_DEEP, 8), PACK_DEEP)
        value = [raw_counts[j, rel, :].astype(jnp.float32) for j in range(tiles)]
        heads = [state[a, 0, here, :] for a in range(arrays - 1)] + [value[0]]
        tails = [state[a, tiles - 1, here, :] for a in range(arrays - 1)] + [value[-1]]
        lp, rp = heads[0], pltpu.roll(tails[0], SEG, 1)
        for a in range(1, arrays):
            lp = jnp.where(seg[:1] == a, pltpu.roll(heads[a], SEG * a, 1), lp)
            rp = jnp.where(seg[:1] == a, pltpu.roll(tails[a], SEG * (a + 1) % LANES, 1), rp)
        left_pack[rel, :] = lp
        right_pack[rel, :] = rp
        for j in range(tiles):
            state[cnt, j, here, :] = value[j]
        both = sum(value)
        return counted + sum(both[8 * u : 8 * u + 8] for u in range(PACK_DEEP // 8))

    zeros = jnp.zeros((8, LANES), jnp.float32)
    counted = lax.fori_loop(0, rows // PACK_DEEP, pack, zeros)

    pl.semaphore_wait(barrier, devices - 1)

    up, down = lax.rem(row + nr - 1, nr), lax.rem(row + 1, nr)
    left, right = lax.rem(col + nc - 1, nc), lax.rem(col + 1, nc)
    head, tail = pl.ds(0, HALO), pl.ds(rows - HALO, HALO)
    body, below = pl.ds(HALO, rows), pl.ds(HALO + rows, HALO)
    halos = [
        (left_pack.at[:, :], from_right.at[body, :], (row, left)),
        (right_pack.at[:, :], from_left.at[body, :], (row, right)),
        (
            state.at[:, pl.ds(0, tiles), pl.ds(TOP, HALO), :],
            state.at[:, pl.ds(0, tiles), pl.ds(TOP + rows, HALO), :],
            (up, col),
        ),
        (
            state.at[:, pl.ds(0, tiles), pl.ds(TOP + rows - HALO, HALO), :],
            state.at[:, pl.ds(0, tiles), pl.ds(PAD, HALO), :],
            (down, col),
        ),
        (left_pack.at[tail, :], from_right.at[head, :], (down, left)),
        (left_pack.at[head, :], from_right.at[below, :], (up, left)),
        (right_pack.at[tail, :], from_left.at[head, :], (down, right)),
        (right_pack.at[head, :], from_left.at[below, :], (up, right)),
    ]
    halos = [
        pltpu.make_async_remote_copy(
            src_ref=s, dst_ref=d, send_sem=halo_send.at[i], recv_sem=halo_recv.at[i],
            device_id=where, device_id_type=MESH,
        )
        for i, (s, d, where) in enumerate(halos)
    ]
    for copy in halos:
        copy.start()
    for copy in halos:
        copy.wait()

    def unpack(i, carry):
        rel = pl.ds(pl.multiple_of(i * UNPACK_DEEP, 8), UNPACK_DEEP)
        here = pl.ds(pl.multiple_of(PAD + i * UNPACK_DEEP, 8), UNPACK_DEEP)
        fr, fl = from_right[rel, :], from_left[rel, :]
        values = []
        for a in range(arrays):
            right_part = pltpu.roll(fr, (LANES - SEG * a) % LANES, 1) if a else fr
            left_part = pltpu.roll(fl, (LANES - SEG * (a + 1)) % LANES, 1)
            left_part = jnp.where(seg[:1] == 7, left_part, 0.0)
            values.append(jnp.where(seg[:1] == 0, right_part, left_part))
        plus = [state[kap, j, here, :] + 4.0 for j in range(tiles)] + [values[kap] + 4.0]
        for a in range(arrays):
            state[a, tiles, here, :] = values[a]
        for j in range(tiles + 1):
            diagonal[j, here, :] = plus[j]
        return carry

    lax.fori_loop(0, (rows + 2 * HALO) // UNPACK_DEEP, unpack, 0)

    def stencil_tiles(r, deep, lane_tiles):
        rowset = pl.ds(r, deep)
        terms, results = [], []
        for c in range(chains):
            full = [state[c, j, rowset, :] for j in range(tiles + 1)]
            used = sorted({(j + s) % (tiles + 1) for j in lane_tiles for s in (-1, 0)})
            to_right = {j: pltpu.roll(full[j], 1, 1) for j in used}
            used = sorted({(j + s) % (tiles + 1) for j in lane_tiles for s in (1, 0)})
            to_left = {j: pltpu.roll(full[j], LANES - 1, 1) for j in used}
            quad = mass = None
            for j in lane_tiles:
                v = full[j]
                beside = jnp.where(first, to_right[(j - 1) % (tiles + 1)], to_right[j])
                beside += jnp.where(last, to_left[(j + 1) % (tiles + 1)], to_left[j])
                beside += state[c, j, pl.ds(r - 1, deep), :] + state[c, j, pl.ds(r + 1, deep), :]
                av = diagonal[j, rowset, :] * v - beside
                ex = jnp.exp(v)
                results.append((c, j, av, ex))
                quad = v * av if quad is None else quad + v * av
                mass = ex if mass is None else mass + ex
            terms += [quad, mass]
        for c, j, av, ex in results:
            applied[c, j, rowset, :] = av
            intensity[c, j, rowset, :] = ex
        return [sum(t[8 * u : 8 * u + 8] for u in range(deep // 8)) for t in terms]

    def own_part():
        def body(i, sums):
            r = pl.multiple_of(TOP + i * OWN_DEEP, 8)
            terms = stencil_tiles(r, OWN_DEEP, range(tiles))
            return tuple(s + t for s, t in zip(sums, terms))

        zero = jnp.zeros((8, LANES), jnp.float32)
        return lax.fori_loop(0, rows // OWN_DEEP, body, (zero,) * (2 * chains))

    def halo_part():
        def side(i, carry):
            stencil_tiles(pl.multiple_of(TOP + i * SIDE_DEEP, 8), SIDE_DEEP, [tiles])
            return carry

        lax.fori_loop(0, rows // SIDE_DEEP, side, 0)
        stencil_tiles(PAD, HALO, range(tiles + 1))
        stencil_tiles(TOP + rows, HALO, range(tiles + 1))

    def whole(x):
        return jnp.sum(jnp.sum(x, axis=0, keepdims=True), axis=1, keepdims=True)

    counted = whole(counted)

    def send(k, sums):
        q0, e0, q1, e1 = [whole(s) for s in sums]
        out = counted
        for i, value in enumerate((q0, q1, e0, e1)):
            out = jnp.where(seg[:1] == i, value, out)
        payload[k] = out
        gathered[k, me] = out
        for d in sorted(range(1, devices), key=lambda d: -min(d, devices - d)):
            pltpu.make_async_remote_copy(
                src_ref=payload.at[k], dst_ref=gathered.at[k, me],
                send_sem=sum_send.at[k], recv_sem=sum_recv.at[k],
                device_id=peer(d), device_id_type=MESH,
            ).start()

    def collect(k):
        bulk = gathered.at[k, pl.ds(0, devices - 1)]
        copy = pltpu.make_async_remote_copy(
            src_ref=bulk, dst_ref=bulk, send_sem=sum_send.at[k], recv_sem=sum_recv.at[k],
            device_id=peer(1), device_id_type=MESH,
        )
        copy.wait_recv()
        return jnp.broadcast_to(jnp.sum(gathered[k], axis=0), (8, LANES))

    def spread(values):
        out = jnp.zeros((8, LANES), jnp.float32)
        for i, value in enumerate(values):
            out = jnp.where(seg == i, value, out)
        return out

    h = [step_size[c] for c in range(chains)]
    hvec = spread([h[0], h[1], h[0], h[1]])
    hyp = spread([hyper[1, 0], hyper[1, 1], hyper[0, 0], hyper[0, 1]])
    vel = spread([velocity[1, 0], velocity[1, 1], velocity[0, 0], velocity[0, 1]])
    is_quad = seg < 2
    coef = jnp.where(is_quad, 0.5 / total, 1.0 / total)

    def accel(summed, expd):
        target = pltpu.roll(summed, LANES - 2 * SEG, 1) * (1.0 / total)
        return coef * expd * summed - jnp.where(is_quad, 0.5, target)

    def pick(x, i):
        return jnp.sum(jnp.where(lane == i * SEG, x, 0.0), axis=1, keepdims=True)

    def weights(expd, scale):
        scaled = expd * hvec * scale
        return [jnp.broadcast_to(pick(scaled, i)[:1], (1, LANES)) for i in range(2 * chains)]

    def kick(r, deep, c, j, w, scale):
        rowset = pl.ds(r, deep)
        m = state[chains + c, j, rowset, :] + (h[c] * scale) * state[cnt, j, rowset, :]
        return m - w[c] * applied[c, j, rowset, :] - w[chains + c] * intensity[c, j, rowset, :]

    def advance(w, scale):
        def body(i, carry):
            rowset = pl.ds(pl.multiple_of(PAD + i * KICK_DEEP, 8), KICK_DEEP)
            moved = []
            for c in range(chains):
                for j in range(tiles + 1):
                    m = kick(rowset.start, KICK_DEEP, c, j, w, scale)
                    moved.append((c, j, m, state[c, j, rowset, :] + h[c] * m))
            for c, j, m, v in moved:
                state[chains + c, j, rowset, :] = m
                state[c, j, rowset, :] = v
            return carry

        lax.fori_loop(0, (rows + 2 * HALO) // KICK_DEEP, body, 0)

    def round_of(k):
        sums = own_part()
        send(k, sums)

    expd = jnp.exp(hyp)
    round_of(0)
    halo_part()
    advance(weights(expd, 0.5), 0.5)
    round_of(1)

    def step(k, carry):
        hyp, vel, expd = carry
        halo_part()
        a = accel(collect(k - 1), expd)
        vel = vel - jnp.where(k == 1, 0.5, 1.0) * hvec * a
        hyp = hyp + hvec * vel
        expd = jnp.exp(hyp)
        advance(weights(expd, 1.0), 1.0)
        round_of(k + 1)
        return hyp, vel, expd

    hyp, vel, expd = lax.fori_loop(1, STEPS, step, (hyp, vel, expd))

    def stores(base, out, start):
        copies = []
        for c in range(chains):
            for j in range(tiles):
                cols = pl.ds(j * LANES, LANES)
                copies.append(
                    pltpu.make_async_copy(
                        state.at[base + c, j, own, :],
                        out.at[c, :, cols],
                        store_sem.at[start + len(copies)],
                    )
                )
        for copy in copies:
            copy.start()
        return copies

    pending = stores(0, latent_out, 0)
    vel = vel - hvec * accel(collect(STEPS - 1), expd)
    hyp = hyp + hvec * vel
    expd = jnp.exp(hyp)
    w = weights(expd, 0.5)

    def final(i, carry):
        rowset = pl.ds(pl.multiple_of(TOP + i * PACK_DEEP, 8), PACK_DEEP)
        moved = []
        for c in range(chains):
            for j in range(tiles):
                moved.append((c, j, kick(rowset.start, PACK_DEEP, c, j, w, 0.5)))
        for c, j, m in moved:
            state[chains + c, j, rowset, :] = m
        return carry

    lax.fori_loop(0, rows // PACK_DEEP, final, 0)
    pending += stores(chains, momentum_out, len(pending))
    vel = vel - 0.5 * hvec * accel(collect(STEPS), expd)

    out_row, out_col = sublane[:2, :2], lane[:2, :2]
    for x, ref in ((hyp, hyper_out), (vel, velocity_out)):
        picks = [pick(x, i)[:2] for i in range(2 * chains)]
        low = jnp.where(out_col == 0, picks[2], picks[3])
        high = jnp.where(out_col == 0, picks[0], picks[1])
        ref[...] = jnp.where(out_row == 0, low, high)
    for copy in pending:
        copy.wait()

    def drain(k, carry):
        bulk = gathered.at[k, pl.ds(0, devices - 1)]
        pltpu.make_async_remote_copy(
            src_ref=bulk, dst_ref=bulk, send_sem=sum_send.at[k], recv_sem=sum_recv.at[k],
            device_id=peer(1), device_id_type=MESH,
        ).wait_send()
        return carry

    lax.fori_loop(0, STEPS + 1, drain, 0)


def hand_out(latent, momentum, hyper, velocity, latent_out, momentum_out, hyper_out, velocity_out, sems):
    copies = [
        pltpu.make_async_copy(latent, latent_out, sems.at[0]),
        pltpu.make_async_copy(momentum, momentum_out, sems.at[1]),
    ]
    for copy in copies:
        copy.start()
    hyper_out[...] = hyper[...]
    velocity_out[...] = velocity[...]
    for copy in copies:
        copy.wait()


def solution(mesh):
    nr, nc = mesh.shape["row"], mesh.shape["col"]
    devices = nr * nc

    def shards(latent, momentum, hyper_params, velocity, step_size, counts, kappa_field):
        chains, rows, cols = latent.shape
        tiles = cols // LANES
        deep = rows + 2 * TOP
        total = float(rows * nr * cols * nc)
        sizes = (nr, nc, chains, rows, tiles, total)
        anywhere = pl.BlockSpec(memory_space=pl.ANY)
        scalars = pl.BlockSpec(memory_space=pltpu.SMEM)
        small = pl.BlockSpec(memory_space=pltpu.VMEM)
        arrays = 2 * chains + 2
        f32 = jnp.float32
        results = pl.pallas_call(
            functools.partial(kernel, sizes),
            out_shape=(
                jax.ShapeDtypeStruct(latent.shape, f32),
                jax.ShapeDtypeStruct(latent.shape, f32),
                jax.ShapeDtypeStruct(hyper_params.shape, f32),
                jax.ShapeDtypeStruct(velocity.shape, f32),
            ),
            in_specs=[anywhere] * 4 + [scalars] * 3,
            out_specs=(anywhere, anywhere, small, small),
            scratch_shapes=[
                pltpu.VMEM((arrays, tiles + 1, deep, LANES), f32),
                pltpu.VMEM((tiles + 1, deep, LANES), f32),
                pltpu.VMEM((chains, tiles + 1, deep, LANES), f32),
                pltpu.VMEM((chains, tiles + 1, deep, LANES), f32),
                pltpu.VMEM((tiles, rows, LANES), jnp.int32),
                pltpu.VMEM((rows, LANES), f32),
                pltpu.VMEM((rows, LANES), f32),
                pltpu.VMEM((rows + 2 * HALO, LANES), f32),
                pltpu.VMEM((rows + 2 * HALO, LANES), f32),
                pltpu.VMEM((STEPS + 1, 1, LANES), f32),
                pltpu.VMEM((STEPS + 1, devices, 1, LANES), f32),
                pltpu.SemaphoreType.DMA((2 * tiles * (chains + 1),)),
                pltpu.SemaphoreType.DMA((2 * tiles * chains,)),
                pltpu.SemaphoreType.DMA((8,)),
                pltpu.SemaphoreType.DMA((8,)),
                pltpu.SemaphoreType.DMA((STEPS + 1,)),
                pltpu.SemaphoreType.DMA((STEPS + 1,)),
            ],
            compiler_params=pltpu.CompilerParams(collective_id=0, has_side_effects=True),
        )(latent, momentum, counts, kappa_field, hyper_params, velocity, step_size)
        return pl.pallas_call(
            hand_out,
            out_shape=[jax.ShapeDtypeStruct(x.shape, f32) for x in results],
            in_specs=[small] * 4,
            out_specs=[anywhere] * 2 + [small] * 2,
            scratch_shapes=[pltpu.SemaphoreType.DMA((2,))],
        )(*results)

    placed = (
        P(None, "row", "col"),
        P(None, "row", "col"),
        P(),
        P(),
        P(),
        P("row", "col"),
        P("row", "col"),
    )
    return jax.shard_map(
        shards,
        mesh=mesh,
        in_specs=placed,
        out_specs=(P(None, "row", "col"), P(None, "row", "col"), P(), P()),
        check_vma=False,
    )
```
